32 devices in a mesh: row: 8 (over y, x, core), col: 4 (over z).
Axes of the slice: x: 2, y: 2, z: 4, core: 2. Of those that a mesh axis runs over, the one named last changes fastest.
Arguments:
- object_slices: float32 [2, 2, 1024, 512], P(None, None, 'row', 'col'), may hold values from -5 to 5
- probe: float32 [2, 256, 256], replicated, may hold values from -6 to 6
- offsets: int32 [8, 4, 1, 2], P('row', 'col'), may hold values from 0 to 127
- residuals: float32 [8, 4, 1, 2, 256, 256], P('row', 'col'), may hold values from -6 to 6
Outputs:
- new_object: float32 [2, 2, 1024, 512], P(None, None, 'row', 'col')
The draws below stay inside these ranges and needn't reach their ends.
All inputs are finite; a program needn't handle non-finite values.
Results may differ from the reference program's by a relative error of at most 0.0003.
Values sent between devices are 32-bit elements; how exact they have to be, the bound alone decides.
No kernel may reach another device: no remote copies, remote signals or barrier semaphores. Data moves between devices by JAX's collectives and lax.ppermute only.
A program may use at most 64 MiB of HBM per device.

```python
import jax
import jax.numpy as jnp
from jax import lax

WIN = 256
NS = 2
POS_DEV = 1
TILE = 128
N_ROW = 8
N_COL = 4


def with_ends(result, own_key, least, largest):
    longest = result.shape.index(max(result.shape))
    spots = []
    for shift in (0, 1):
        where = [jax.random.randint(jax.random.fold_in(own_key, axis), (), 0, length) for axis, length in enumerate(result.shape)]
        where[longest] = (where[longest] + shift) % result.shape[longest]
        spots.append(tuple(where))
    return result.at[spots[0]].set(least).at[spots[1]].set(largest)


def levels(key, extent, shards, least, largest):
    level, own = 1.0, jax.random.fold_in(key, 6)
    for axis_at, blocks in shards:
        draws = jnp.exp(jax.random.uniform(jax.random.fold_in(own, axis_at), (blocks,), jnp.float32, least / len(shards), largest / len(shards)))
        level = level * jnp.repeat(draws, extent[axis_at] // blocks).reshape([-1 if axis == axis_at else 1 for axis in range(len(extent))])
    return level


def scatter_about(key, extent, deviation, bound, cuts=(), kind=jnp.bfloat16):
    gain = levels(key, extent, cuts, -0.22, 0.18) if cuts else 1.0
    drawn = jax.random.normal(key, extent, jnp.float32) * deviation * gain
    return jnp.minimum(jnp.maximum(drawn, -bound), bound).astype(kind)


def setup_inputs(seed: int = 0) -> dict:
    arg_keys = jax.random.split(jax.random.key(seed), 5)
    object_slices = scatter_about(arg_keys[0], (NS, 2, TILE * N_ROW, TILE * N_COL), 0.7, 5.0, ((2, 8), (3, 4)), jnp.float32)
    probe = scatter_about(arg_keys[1], (2, WIN, WIN), 1.0, 6.0, (), jnp.float32)
    offsets = with_ends(jax.random.randint(arg_keys[2], (N_ROW, N_COL, POS_DEV, 2), 0, TILE), jax.random.fold_in(arg_keys[2], 1), 0, TILE - 1).astype(jnp.int32)
    residuals = scatter_about(arg_keys[3], (N_ROW, N_COL, POS_DEV, 2, WIN, WIN), 1.0, 6.0, ((0, 8), (1, 4)), jnp.float32)
    return dict(object_slices=object_slices, probe=probe, offsets=offsets, residuals=residuals)


FRESNEL = 40.0
STEP_SIZE = 0.5
REGULAR = 1.0


def kernel_phase():
    index = jnp.arange(WIN, dtype=jnp.int32)
    freq = jnp.where(index < WIN // 2, index, index - WIN).astype(jnp.float32) / WIN
    phase = FRESNEL * jnp.pi * freq * freq
    return phase[:, None] + phase[None, :]


def propagate(wave, phase, direction):
    spectrum = jnp.fft.fft2(wave, norm="ortho")
    return jnp.fft.ifft2(spectrum * jnp.exp(-1j * direction * phase), norm="ortho")


def one_position(window, probe_wave, resid, phase):
    waves = [probe_wave]
    wave = probe_wave
    for layer in range(NS - 1):
        wave = propagate(wave * window[layer], phase, 1.0)
        waves.append(wave)
    back = jnp.fft.ifft2(resid, norm="ortho")
    parts = [None] * NS
    for layer in reversed(range(NS)):
        current = waves[layer]
        term = jnp.conj(current) * back
        light = jnp.real(current) * jnp.real(current) + jnp.imag(current) * jnp.imag(current)
        parts[layer] = jnp.stack([jnp.real(term), jnp.imag(term), light])
        if layer > 0:
            back = propagate(jnp.conj(window[layer]) * back, phase, -1.0)
    return jnp.stack(parts)


def reference(object_slices, probe, offsets, residuals):
    height = TILE * N_ROW
    breadth = TILE * N_COL
    whole = object_slices[:, 0] + 1j * object_slices[:, 1]
    padded = jnp.concatenate([whole, whole[:, :2 * TILE]], axis=1)
    padded = jnp.concatenate([padded, padded[:, :, :2 * TILE]], axis=2)
    probe_wave = probe[0] + 1j * probe[1]
    phase = kernel_phase()
    buffer = jnp.zeros((NS, 3, height + 2 * TILE, breadth + 2 * TILE), jnp.float32)

    def visit(buffer, tile_id):
        tile_row = tile_id // N_COL
        tile_col = tile_id % N_COL
        zero = jnp.zeros((), jnp.int32)
        for slot in range(POS_DEV):
            top = (tile_row * TILE + offsets[tile_row, tile_col, slot, 0]).astype(jnp.int32)
            left = (tile_col * TILE + offsets[tile_row, tile_col, slot, 1]).astype(jnp.int32)
            window = lax.dynamic_slice(padded, (zero, top, left), (NS, WIN, WIN))
            pair = residuals[tile_row, tile_col, slot]
            resid = pair[0] + 1j * pair[1]
            contrib = one_position(window, probe_wave, resid, phase).astype(jnp.float32)
            older = lax.dynamic_slice(buffer, (zero, zero, top, left), (NS, 3, WIN, WIN))
            buffer = lax.dynamic_update_slice(buffer, older + contrib, (zero, zero, top, left))
        return buffer, None

    tiles = jnp.arange(N_ROW * N_COL, dtype=jnp.int32)
    buffer, unused = lax.scan(visit, buffer, tiles)
    buffer = buffer.at[:, :, :2 * TILE].add(buffer[:, :, height:])
    buffer = buffer[:, :, :height]
    buffer = buffer.at[:, :, :, :2 * TILE].add(buffer[:, :, :, breadth:])
    buffer = buffer[:, :, :, :breadth]
    gradient = buffer[:, 0:2]
    illumination = buffer[:, 2:3]
    return object_slices - STEP_SIZE * gradient / (illumination + REGULAR)
```

```python
import math

import jax
import jax.numpy as jnp
import numpy as np
from jax import lax
from jax.sharding import PartitionSpec as P

FRESNEL = 40.0
STEP_SIZE = 0.5
REGULAR = 1.0


def moved(value, axis, steps):
    count = lax.axis_size(axis)
    return lax.ppermute(value, axis, [(k, (k + steps) % count) for k in range(count)])


def tables(width):
    index = np.arange(width)
    inverse = np.exp(2j * np.pi / width * (index[:, None] * index[None, :] % width)) / math.sqrt(width)
    freq = np.where(index < width // 2, index, index - width) / width
    phase = FRESNEL * np.pi * freq * freq
    prop = (inverse * np.exp(-1j * phase)[None, :]) @ np.conj(inverse)
    return inverse, prop


def sandwich(mat, wave_re, wave_im):
    re, im = jnp.asarray(mat.real, jnp.float32), jnp.asarray(mat.imag, jnp.float32)
    right = jnp.block([[re, im], [-im, re]])
    left = jnp.block([[re, -im], [im, re]])
    width = re.shape[0]
    dot = lambda a, b: jnp.dot(a, b, precision=lax.Precision.HIGH, preferred_element_type=jnp.float32)
    half = dot(jnp.concatenate([wave_re, wave_im], axis=1), right)
    full = dot(left, jnp.concatenate([half[:, :width], half[:, width:]], axis=0))
    return full[:width], full[width:]


def columns(region, left, width):
    return lax.dynamic_slice_in_dim(region, left, width, axis=2)


def rows(up, own, down, top, width):
    return lax.dynamic_slice_in_dim(jnp.concatenate([up, own, down], axis=1), top, width, axis=1)


def placed(value, at, axis, tile):
    pads = [(0, 0)] * value.ndim
    pads[axis] = (tile, tile)
    return lax.dynamic_slice_in_dim(jnp.pad(value, pads), tile - at, 3 * tile, axis=axis)


def local(object_slices, probe, offsets, residuals):
    layers, _, tile, _ = object_slices.shape
    width = probe.shape[1]
    inverse, prop = tables(width)

    off = [offsets, moved(offsets, "row", 1), moved(offsets, "row", 2)]
    resid = moved(residuals[0, 0, 0], "row", 1)
    tops = [o[0, 0, 0, 0] for o in off]
    lefts = [o[0, 0, 0, 1] for o in off]

    near = [moved(object_slices[s], "col", -1) for s in range(layers)]
    far = [moved(n, "col", -1) for n in near]
    window = []
    for s in range(layers):
        region = jnp.concatenate([object_slices[s], near[s], far[s]], axis=2)
        up = moved(columns(region, lefts[0], width), "row", 1)
        down = moved(columns(region, lefts[2], width), "row", -1)
        window.append(rows(up, columns(region, lefts[1], width), down, tops[1], width))

    back_re, back_im = sandwich(inverse, resid[0], resid[1])

    def shared(terms):
        lifted = placed(terms, tops[1], 1, tile)
        above = moved(lifted[:, :tile], "row", -1)
        below = moved(lifted[:, 2 * tile :], "row", 1)
        strip = (
            placed(above, lefts[0], 2, tile)
            + placed(lifted[:, tile : 2 * tile], lefts[1], 2, tile)
            + placed(below, lefts[2], 2, tile)
        )
        total = strip[:, :, 2 * tile :]
        for band in (1, 0):
            total = moved(total, "col", 1) + strip[:, :, band * tile : (band + 1) * tile]
        return total

    trans_re, trans_im = window[0]
    wave_re, wave_im = sandwich(
        prop, probe[0] * trans_re - probe[1] * trans_im, probe[0] * trans_im + probe[1] * trans_re
    )
    second = shared(
        jnp.stack(
            [
                wave_re * back_re + wave_im * back_im,
                wave_re * back_im - wave_im * back_re,
                wave_re * wave_re + wave_im * wave_im,
            ]
        )
    )
    trans_re, trans_im = window[1]
    pulled_re, pulled_im = sandwich(
        np.conj(prop), trans_re * back_re + trans_im * back_im, trans_re * back_im - trans_im * back_re
    )
    first = shared(
        jnp.stack([probe[0] * pulled_re + probe[1] * pulled_im, probe[0] * pulled_im - probe[1] * pulled_re])
    )

    light = probe[0] * probe[0] + probe[1] * probe[1]
    offs = jnp.stack([o[0, 0, 0] for o in off])
    all_offs = [offs, moved(offs, "col", 1), moved(offs, "col", 2)]
    spread = jnp.pad(light, tile)
    bright = jnp.zeros((tile, tile), jnp.float32)
    for across in range(3):
        for along in range(3):
            at = all_offs[across][along]
            bright += lax.dynamic_slice(
                spread, (tile * (along + 1) - at[0], tile * (across + 1) - at[1]), (tile, tile)
            )
    new0 = object_slices[0] - STEP_SIZE * first / (bright + REGULAR)
    new1 = object_slices[1] - STEP_SIZE * second[:2] / (second[2:] + REGULAR)
    return jnp.stack([new0, new1])


def solution(mesh):
    split = (
        P(None, None, "row", "col"),
        P(),
        P("row", "col", None, None),
        P("row", "col", None, None, None, None),
    )
    return jax.shard_map(local, mesh=mesh, in_specs=split, out_specs=split[0], check_vma=False)
```

```python
import functools
import math

import jax
import jax.numpy as jnp
import numpy as np
from jax import lax
from jax.experimental import pallas as pl
from jax.experimental.pallas import tpu as pltpu
from jax.sharding import PartitionSpec as P

FRESNEL = 40.0
STEP_SIZE = 0.5
REGULAR = 1.0
VMEM_BYTES = 16 * 2**20
VMEM = pl.BlockSpec(memory_space=pltpu.VMEM)
SMEM = pl.BlockSpec(memory_space=pltpu.SMEM)


def moved(value, axis, steps):
    count = lax.axis_size(axis)
    return lax.ppermute(value, axis, [(k, (k + steps) % count) for k in range(count)])


def call(body, name, out_shapes, ins, scratch=()):
    return pl.pallas_call(
        body,
        name=name,
        out_shape=[jax.ShapeDtypeStruct(s, d) for s, d in out_shapes],
        in_specs=[SMEM if v.dtype == jnp.int32 else VMEM for v in ins],
        out_specs=[VMEM] * len(out_shapes),
        scratch_shapes=list(scratch),
        compiler_params=pltpu.CompilerParams(vmem_limit_bytes=VMEM_BYTES),
    )(*ins)


def halves(value):
    high = value.astype(jnp.bfloat16)
    return high, (value - high.astype(jnp.float32)).astype(jnp.bfloat16)


def tables(width):
    index = np.arange(width)
    inverse = np.exp(2j * np.pi / width * (index[:, None] * index[None, :] % width)) / math.sqrt(width)
    freq = np.where(index < width // 2, index, index - width) / width
    phase = FRESNEL * np.pi * freq * freq
    prop = (inverse * np.exp(-1j * phase)[None, :]) @ np.conj(inverse)

    def packed(mat):
        parts = []
        for part in (mat.real, mat.imag):
            part = part.astype(np.float32)
            high = part.astype(jnp.bfloat16)
            parts.append(np.stack([high, (part - high.astype(np.float32)).astype(jnp.bfloat16)]))
        return jnp.asarray(np.stack(parts))

    return packed(inverse), packed(prop)


def dot3(left, right):
    dot = functools.partial(jnp.dot, preferred_element_type=jnp.float32)
    return dot(left[0], right[0]) + dot(left[1], right[0]) + dot(left[0], right[1])


def sandwich(mat_ref, sign, wave_re, wave_im):
    mat_re = (mat_ref[0, 0], mat_ref[0, 1])
    mat_im = (mat_ref[1, 0], mat_ref[1, 1])
    wave_re, wave_im = halves(wave_re), halves(wave_im)
    half_re = dot3(wave_re, mat_re) - sign * dot3(wave_im, mat_im)
    half_im = dot3(wave_im, mat_re) + sign * dot3(wave_re, mat_im)
    half_re, half_im = halves(half_re), halves(half_im)
    return (
        dot3(mat_re, half_re) - sign * dot3(mat_im, half_im),
        dot3(mat_re, half_im) + sign * dot3(mat_im, half_re),
    )


def lanes(shape):
    return lax.broadcasted_iota(jnp.int32, shape, len(shape) - 1)


def turned(value, by):
    return pltpu.roll(value, by, value.ndim - 1)


def back_body(resid_ref, mat_ref, back_ref):
    back_ref[0], back_ref[1] = sandwich(mat_ref, 1.0, resid_ref[0], resid_ref[1])


def spread_body(off0, off1, off2, own_ref, near_ref, far_ref, up_ref, mid_ref, down_ref):
    tile = own_ref.shape[-1]
    for off, out_ref in ((off0, up_ref), (off1, mid_ref), (off2, down_ref)):
        left = off[0, 1]
        by = lax.select(left == 0, 0, tile - left)
        keep = lanes((tile, tile)) < tile - left
        for part in range(own_ref.shape[0]):
            first, second, third = (turned(ref[part], by) for ref in (own_ref, near_ref, far_ref))
            out_ref[part, :, :tile] = jnp.where(keep, first, second)
            out_ref[part, :, tile:] = jnp.where(keep, second, third)


def rows_at(ref, start, count):
    rest = lax.rem(start, 8)
    value = ref[pl.ds(pl.multiple_of(start - rest, 8), count + 8)]
    value = value.reshape(count // 8 + 1, 8, value.shape[-1])
    value = pltpu.roll(value, lax.rem(8 - rest, 8), 1)
    keep = lax.broadcasted_iota(jnp.int32, value[1:].shape, 1) < 8 - rest
    return jnp.where(keep, value[:-1], value[1:]).reshape(count, value.shape[-1])


def rows_to(ref, start, value):
    count, width = value.shape
    rest = lax.rem(start, 8)
    value = pltpu.roll(value.reshape(count // 8, 8, width), rest, 1)
    none = jnp.zeros((1, 8, width), value.dtype)
    now, before = jnp.concatenate([value, none], axis=0), jnp.concatenate([none, value], axis=0)
    keep = lax.broadcasted_iota(jnp.int32, now.shape, 1) >= rest
    ref[pl.ds(pl.multiple_of(start - rest, 8), count + 8)] = jnp.where(keep, now, before).reshape(count + 8, width)


def windowed(tall_ref, top, up_ref, mid_ref, down_ref):
    tile, width = up_ref.shape[1:]
    for band, ref in enumerate((up_ref, mid_ref, down_ref)):
        tall_ref[:2, band * tile : (band + 1) * tile] = ref[...]
    return rows_at(tall_ref.at[0], top, width), rows_at(tall_ref.at[1], top, width)


def handed_out(tall_ref, top, terms, outs):
    tile, width = outs[0].shape[1:]
    zeros = jnp.zeros((tile, width), jnp.float32)
    for part, term in enumerate(terms):
        tall_ref[part, :tile] = zeros
        tall_ref[part, 2 * tile :] = zeros
        rows_to(tall_ref.at[part], top, term)
        for band, out_ref in enumerate(outs):
            out_ref[part] = tall_ref[part, band * tile : (band + 1) * tile]


def wave_body(off1, up_ref, mid_ref, down_ref, probe_ref, back_ref, mat_ref, out0, out1, out2, tall_ref):
    top = off1[0, 0]
    trans_re, trans_im = windowed(tall_ref, top, up_ref, mid_ref, down_ref)
    probe_re, probe_im = probe_ref[0], probe_ref[1]
    wave_re, wave_im = sandwich(
        mat_ref, 1.0, probe_re * trans_re - probe_im * trans_im, probe_re * trans_im + probe_im * trans_re
    )
    back_re, back_im = back_ref[0], back_ref[1]
    terms = (
        wave_re * back_re + wave_im * back_im,
        wave_re * back_im - wave_im * back_re,
        wave_re * wave_re + wave_im * wave_im,
    )
    handed_out(tall_ref, top, terms, (out0, out1, out2))


def pull_body(off1, up_ref, mid_ref, down_ref, probe_ref, back_ref, mat_ref, out0, out1, out2, tall_ref):
    top = off1[0, 0]
    trans_re, trans_im = windowed(tall_ref, top, up_ref, mid_ref, down_ref)
    back_re, back_im = back_ref[0], back_ref[1]
    pulled_re, pulled_im = sandwich(
        mat_ref, -1.0, trans_re * back_re + trans_im * back_im, trans_re * back_im - trans_im * back_re
    )
    probe_re, probe_im = probe_ref[0], probe_ref[1]
    terms = (probe_re * pulled_re + probe_im * pulled_im, probe_re * pulled_im - probe_im * pulled_re)
    handed_out(tall_ref, top, terms, (out0, out1, out2))


def merge_body(off0, off1, off2, above_ref, mid_ref, below_ref, out0, out1, out2):
    tile = out0.shape[-1]
    for part in range(out0.shape[0]):
        totals = [jnp.zeros((tile, tile), jnp.float32) for _ in range(3)]
        for off, ref in ((off0, above_ref), (off1, mid_ref), (off2, below_ref)):
            left = off[0, 1]
            first, second = turned(ref[part, :, :tile], left), turned(ref[part, :, tile:], left)
            inside = lanes((tile, tile)) >= left
            totals[0] += jnp.where(inside, first, 0.0)
            totals[1] += jnp.where(inside, second, first)
            totals[2] += jnp.where(inside, 0.0, second)
        out0[part], out1[part], out2[part] = totals


def bright_body(offs0, offs1, offs2, probe_ref, out_ref, tall_ref):
    tile = out_ref.shape[-1]
    width = probe_ref.shape[-1]
    tall_ref[:tile] = jnp.zeros((tile, width), jnp.float32)
    tall_ref[tile + width :] = jnp.zeros((tile + 8, width), jnp.float32)
    tall_ref[tile : tile + width] = probe_ref[0] * probe_ref[0] + probe_ref[1] * probe_ref[1]
    total = jnp.zeros((tile, tile), jnp.float32)
    for across, offs in enumerate((offs0, offs1, offs2)):
        for along in range(3):
            top, left = offs[along, 0], offs[along, 1]
            strip = rows_at(tall_ref, tile * (along + 1) - top, tile)
            inside = lanes((tile, tile)) >= left
            first, second = turned(strip[:, :tile], left), turned(strip[:, tile:], left)
            if across == 0:
                total += jnp.where(inside, first, 0.0)
            elif across == 1:
                total += jnp.where(inside, second, first)
            else:
                total += jnp.where(inside, 0.0, second)
    out_ref[...] = total


def joined_body(off0, off1, off2, out_ref):
    for along, off in enumerate((off0, off1, off2)):
        out_ref[along, 0] = off[0, 0]
        out_ref[along, 1] = off[0, 1]


def local(object_slices, probe, offsets, residuals):
    layers, _, tile, _ = object_slices.shape
    width = probe.shape[1]
    inverse, prop = tables(width)
    f32 = jnp.float32

    off = offsets.reshape(1, 2)
    off = [off, moved(off, "row", 1), moved(off, "row", 2)]
    near = [moved(object_slices[s], "col", -1) for s in range(layers)]
    resid = moved(residuals.reshape(2, width, width), "row", 1)
    far = [moved(n, "col", -1) for n in near]

    (back,) = call(back_body, "back", [((2, width, width), f32)], [resid, inverse])

    def window(s):
        strip = ((2, tile, width), f32)
        up, mid, down = call(spread_body, "spread", [strip] * 3, [*off, object_slices[s], near[s], far[s]])
        return moved(up, "row", 1), mid, moved(down, "row", -1)

    def terms(body, name, parts, strips):
        tall = pltpu.VMEM((3, 3 * tile, width), f32)
        strip = ((parts, tile, width), f32)
        return call(body, name, [strip] * 3, [off[1], *strips, probe, back, prop], [tall])

    def shared(lifted):
        above, below = moved(lifted[0], "row", -1), moved(lifted[2], "row", 1)
        band = (lifted[1].shape[0], tile, tile)
        first, second, third = call(merge_body, "merge", [(band, f32)] * 3, [*off, above, lifted[1], below])
        return first + moved(second + moved(third, "col", 1), "col", 1)

    strips = [window(s) for s in range(layers)]
    second = shared(terms(wave_body, "wave", 3, strips[0]))
    first = shared(terms(pull_body, "pull", 2, strips[1]))

    offs = pl.pallas_call(
        joined_body,
        name="joined",
        out_shape=jax.ShapeDtypeStruct((3, 2), jnp.int32),
        in_specs=[SMEM] * 3,
        out_specs=SMEM,
        compiler_params=pltpu.CompilerParams(vmem_limit_bytes=VMEM_BYTES),
    )(*off)
    tall = pltpu.VMEM((2 * tile + width + 8, width), f32)
    (bright,) = call(
        bright_body, "bright", [((tile, tile), f32)], [offs, moved(offs, "col", 1), moved(offs, "col", 2), probe], [tall]
    )

    new0 = object_slices[0] - STEP_SIZE * first / (bright + REGULAR)
    new1 = object_slices[1] - STEP_SIZE * second[:2] / (second[2:] + REGULAR)
    return jnp.stack([new0, new1])


def solution(mesh):
    split = (
        P(None, None, "row", "col"),
        P(),
        P("row", "col", None, None),
        P("row", "col", None, None, None, None),
    )
    return jax.shard_map(local, mesh=mesh, in_specs=split, out_specs=split[0], check_vma=False)
```

```python
import functools
import math

import jax
import jax.numpy as jnp
import numpy as np
from jax import lax
from jax.experimental import pallas as pl
from jax.experimental.pallas import tpu as pltpu
from jax.sharding import PartitionSpec as P


FRESNEL = 40.0
STEP_SIZE = 0.5
REGULAR = 1.0
VMEM_BYTES = 16 * 2**20
VMEM = pl.BlockSpec(memory_space=pltpu.VMEM)


def moved(value, axis, steps):
    count = lax.axis_size(axis)
    return lax.ppermute(value, axis, [(k, (k + steps) % count) for k in range(count)])


def call(body, out_shapes, ins, scratch=()):
    return pl.pallas_call(
        body,
        out_shape=[jax.ShapeDtypeStruct(s, d) for s, d in out_shapes],
        in_specs=[VMEM] * len(ins),
        out_specs=[VMEM] * len(out_shapes),
        scratch_shapes=list(scratch),
        compiler_params=pltpu.CompilerParams(vmem_limit_bytes=VMEM_BYTES),
    )(*ins)


def halves(value):
    high = value.astype(jnp.bfloat16)
    return high, (value - high.astype(jnp.float32)).astype(jnp.bfloat16)


def tables(width):
    index = np.arange(width)
    inverse = np.exp(2j * np.pi / width * (index[:, None] * index[None, :] % width)) / math.sqrt(width)
    freq = np.where(index < width // 2, index, index - width) / width
    phase = FRESNEL * np.pi * freq * freq
    prop = (inverse * np.exp(-1j * phase)[None, :]) @ np.conj(inverse)

    def packed(mat):
        parts = []
        for part in (mat.real, mat.imag):
            part = part.astype(np.float32)
            high = part.astype(jnp.bfloat16)
            parts.append(np.stack([high, (part - high.astype(np.float32)).astype(jnp.bfloat16)]))
        return jnp.asarray(np.stack(parts))

    return packed(inverse), packed(prop)


def dot3(left, right):
    dot = functools.partial(jnp.dot, preferred_element_type=jnp.float32)
    return dot(left[0], right[0]) + dot(left[1], right[0]) + dot(left[0], right[1])


def sandwich(mat_ref, sign, wave_re, wave_im):
    mat_re = (mat_ref[0, 0], mat_ref[0, 1])
    mat_im = (mat_ref[1, 0], mat_ref[1, 1])
    wave_re, wave_im = halves(wave_re), halves(wave_im)
    half_re = dot3(wave_re, mat_re) - sign * dot3(wave_im, mat_im)
    half_im = dot3(wave_im, mat_re) + sign * dot3(wave_re, mat_im)
    half_re, half_im = halves(half_re), halves(half_im)
    return (
        dot3(mat_re, half_re) - sign * dot3(mat_im, half_im),
        dot3(mat_re, half_im) + sign * dot3(mat_im, half_re),
    )


def lanes(shape):
    return lax.broadcasted_iota(jnp.int32, shape, len(shape) - 1)


def turned(value, by):
    return pltpu.roll(value, by, value.ndim - 1)


def back_body(resid_ref, mat_ref, back_ref):
    back_ref[0], back_ref[1] = sandwich(mat_ref, 1.0, resid_ref[0], resid_ref[1])


def spread_body(off0, off1, off2, own_ref, near_ref, far_ref, up_ref, mid_ref, down_ref):
    tile = own_ref.shape[-1]
    for off, out_ref in ((off0, up_ref), (off1, mid_ref), (off2, down_ref)):
        left = off[0, 1]
        by = lax.select(left == 0, 0, tile - left)
        keep = lanes((tile, tile)) < tile - left
        for part in range(own_ref.shape[0]):
            first, second, third = (turned(ref[part], by) for ref in (own_ref, near_ref, far_ref))
            out_ref[part, :, :tile] = jnp.where(keep, first, second)
            out_ref[part, :, tile:] = jnp.where(keep, second, third)


def rows_at(ref, start, count):
    rest = lax.rem(start, 8)
    value = ref[pl.ds(pl.multiple_of(start - rest, 8), count + 8)]
    value = value.reshape(count // 8 + 1, 8, value.shape[-1])
    value = pltpu.roll(value, lax.rem(8 - rest, 8), 1)
    keep = lax.broadcasted_iota(jnp.int32, value[1:].shape, 1) < 8 - rest
    return jnp.where(keep, value[:-1], value[1:]).reshape(count, value.shape[-1])


def rows_to(ref, start, value):
    count, width = value.shape
    rest = lax.rem(start, 8)
    value = pltpu.roll(value.reshape(count // 8, 8, width), rest, 1)
    none = jnp.zeros((1, 8, width), value.dtype)
    now, before = jnp.concatenate([value, none], axis=0), jnp.concatenate([none, value], axis=0)
    keep = lax.broadcasted_iota(jnp.int32, now.shape, 1) >= rest
    ref[pl.ds(pl.multiple_of(start - rest, 8), count + 8)] = jnp.where(keep, now, before).reshape(count + 8, width)


def windowed(tall_ref, top, up_ref, mid_ref, down_ref):
    tile, width = up_ref.shape[1:]
    for band, ref in enumerate((up_ref, mid_ref, down_ref)):
        tall_ref[:2, band * tile : (band + 1) * tile] = ref[...]
    return rows_at(tall_ref.at[0], top, width), rows_at(tall_ref.at[1], top, width)


def handed_out(tall_ref, top, terms, outs):
    tile, width = outs[0].shape[1:]
    zeros = jnp.zeros((tile, width), jnp.float32)
    for part, term in enumerate(terms):
        tall_ref[part, :tile] = zeros
        tall_ref[part, 2 * tile :] = zeros
        rows_to(tall_ref.at[part], top, term)
        for band, out_ref in enumerate(outs):
            out_ref[part] = tall_ref[part, band * tile : (band + 1) * tile]


def wave_body(off1, up_ref, mid_ref, down_ref, probe_ref, back_ref, mat_ref, out0, out1, out2, tall_ref):
    top = off1[0, 0]
    trans_re, trans_im = windowed(tall_ref, top, up_ref, mid_ref, down_ref)
    probe_re, probe_im = probe_ref[0], probe_ref[1]
    wave_re, wave_im = sandwich(
        mat_ref, 1.0, probe_re * trans_re - probe_im * trans_im, probe_re * trans_im + probe_im * trans_re
    )
    back_re, back_im = back_ref[0], back_ref[1]
    terms = (
        wave_re * back_re + wave_im * back_im,
        wave_re * back_im - wave_im * back_re,
        wave_re * wave_re + wave_im * wave_im,
    )
    handed_out(tall_ref, top, terms, (out0, out1, out2))


def pull_body(off1, up_ref, mid_ref, down_ref, probe_ref, back_ref, mat_ref, out0, out1, out2, tall_ref):
    top = off1[0, 0]
    trans_re, trans_im = windowed(tall_ref, top, up_ref, mid_ref, down_ref)
    back_re, back_im = back_ref[0], back_ref[1]
    pulled_re, pulled_im = sandwich(
        mat_ref, -1.0, trans_re * back_re + trans_im * back_im, trans_re * back_im - trans_im * back_re
    )
    probe_re, probe_im = probe_ref[0], probe_ref[1]
    terms = (probe_re * pulled_re + probe_im * pulled_im, probe_re * pulled_im - probe_im * pulled_re)
    handed_out(tall_ref, top, terms, (out0, out1, out2))


def merge_body(off0, off1, off2, above_ref, mid_ref, below_ref, out0, out1, out2):
    tile = out0.shape[-1]
    for part in range(out0.shape[0]):
        totals = [jnp.zeros((tile, tile), jnp.float32) for _ in range(3)]
        for off, ref in ((off0, above_ref), (off1, mid_ref), (off2, below_ref)):
            left = off[0, 1]
            first, second = turned(ref[part, :, :tile], left), turned(ref[part, :, tile:], left)
            inside = lanes((tile, tile)) >= left
            totals[0] += jnp.where(inside, first, 0.0)
            totals[1] += jnp.where(inside, second, first)
            totals[2] += jnp.where(inside, 0.0, second)
        out0[part], out1[part], out2[part] = totals


def bright_body(offs0, offs1, offs2, probe_ref, out_ref, tall_ref):
    tile = out_ref.shape[-1]
    width = probe_ref.shape[-1]
    tall_ref[:tile] = jnp.zeros((tile, width), jnp.float32)
    tall_ref[tile + width :] = jnp.zeros((tile + 8, width), jnp.float32)
    tall_ref[tile : tile + width] = probe_ref[0] * probe_ref[0] + probe_ref[1] * probe_ref[1]
    total = jnp.zeros((tile, tile), jnp.float32)
    for across, offs in enumerate((offs0, offs1, offs2)):
        for along in range(3):
            top, left = offs[along, 0], offs[along, 1]
            strip = rows_at(tall_ref, tile * (along + 1) - top, tile)
            inside = lanes((tile, tile)) >= left
            first, second = turned(strip[:, :tile], left), turned(strip[:, tile:], left)
            if across == 0:
                total += jnp.where(inside, first, 0.0)
            elif across == 1:
                total += jnp.where(inside, second, first)
            else:
                total += jnp.where(inside, 0.0, second)
    out_ref[...] = total


def joined_body(off0, off1, off2, out_ref):
    for along, off in enumerate((off0, off1, off2)):
        out_ref[along : along + 1] = off[...]


def local(object_slices, probe, offsets, residuals):
    layers, _, tile, _ = object_slices.shape
    width = probe.shape[1]
    inverse, prop = tables(width)
    f32 = jnp.float32

    off = offsets.reshape(1, 2)
    off = [off, moved(off, "row", 1), moved(off, "row", 2)]
    near = [moved(object_slices[s], "col", -1) for s in range(layers)]
    resid = moved(residuals.reshape(2, width, width), "row", 1)
    far = [moved(n, "col", -1) for n in near]

    (back,) = call(back_body, [((2, width, width), f32)], [resid, inverse])

    def window(s):
        strip = ((2, tile, width), f32)
        up, mid, down = call(spread_body, [strip] * 3, [*off, object_slices[s], near[s], far[s]])
        return moved(up, "row", 1), mid, moved(down, "row", -1)

    def terms(body, parts, strips):
        tall = pltpu.VMEM((3, 3 * tile, width), f32)
        strip = ((parts, tile, width), f32)
        return call(body, [strip] * 3, [off[1], *strips, probe, back, prop], [tall])

    def shared(lifted):
        above, below = moved(lifted[0], "row", -1), moved(lifted[2], "row", 1)
        band = (lifted[1].shape[0], tile, tile)
        first, second, third = call(merge_body, [(band, f32)] * 3, [*off, above, lifted[1], below])
        return first + moved(second + moved(third, "col", 1), "col", 1)

    strips = [window(s) for s in range(layers)]
    second = shared(terms(wave_body, 3, strips[0]))
    first = shared(terms(pull_body, 2, strips[1]))

    (offs,) = call(joined_body, [((3, 2), jnp.int32)], off)
    tall = pltpu.VMEM((2 * tile + width + 8, width), f32)
    (bright,) = call(
        bright_body, [((tile, tile), f32)], [offs, moved(offs, "col", 1), moved(offs, "col", 2), probe], [tall]
    )

    new0 = object_slices[0] - STEP_SIZE * first / (bright + REGULAR)
    new1 = object_slices[1] - STEP_SIZE * second[:2] / (second[2:] + REGULAR)
    return jnp.stack([new0, new1])


def solution(mesh):
    split = (
        P(None, None, "row", "col"),
        P(),
        P("row", "col", None, None),
        P("row", "col", None, None, None, None),
    )

    return jax.shard_map(local, mesh=mesh, in_specs=split, out_specs=split[0], check_vma=False)
```

```python
import functools
import math

import jax
import jax.numpy as jnp
import numpy as np
from jax import lax
from jax.experimental import pallas as pl
from jax.experimental.pallas import tpu as pltpu
from jax.sharding import PartitionSpec as P


FRESNEL = 40.0
STEP_SIZE = 0.5
REGULAR = 1.0
VMEM_BYTES = 16 * 2**20
VMEM = pl.BlockSpec(memory_space=pltpu.VMEM)


def moved(value, axis, steps):
    count = lax.axis_size(axis)
    return lax.ppermute(value, axis, [(k, (k + steps) % count) for k in range(count)])


def swapped(value):
    return lax.ppermute(value, "row", [(k, k ^ 1) for k in range(lax.axis_size("row"))])


def is_even():
    return lax.rem(lax.axis_index("row"), 2) == 0


def call(body, out_shapes, ins, scratch=()):
    return pl.pallas_call(
        body,
        out_shape=[jax.ShapeDtypeStruct(s, d) for s, d in out_shapes],
        in_specs=[VMEM] * len(ins),
        out_specs=[VMEM] * len(out_shapes),
        scratch_shapes=list(scratch),
        compiler_params=pltpu.CompilerParams(vmem_limit_bytes=VMEM_BYTES),
    )(*ins)


def halves(value):
    high = value.astype(jnp.bfloat16)
    return high, (value - high.astype(jnp.float32)).astype(jnp.bfloat16)


def tables(width):
    index = np.arange(width)
    inverse = np.exp(2j * np.pi / width * (index[:, None] * index[None, :] % width)) / math.sqrt(width)
    freq = np.where(index < width // 2, index, index - width) / width
    phase = FRESNEL * np.pi * freq * freq
    prop = (inverse * np.exp(-1j * phase)[None, :]) @ np.conj(inverse)

    def packed(mat):
        parts = []
        for part in (mat.real, mat.imag):
            part = part.astype(np.float32)
            high = part.astype(jnp.bfloat16)
            parts.append(np.stack([high, (part - high.astype(np.float32)).astype(jnp.bfloat16)]))
        return jnp.asarray(np.stack(parts))

    return packed(inverse), packed(prop)


def dot3(left, right):
    dot = functools.partial(jnp.dot, preferred_element_type=jnp.float32)
    return dot(left[0], right[0]) + dot(left[1], right[0]) + dot(left[0], right[1])


def sandwich(mat_ref, sign, wave_re, wave_im):
    mat_re = (mat_ref[0, 0], mat_ref[0, 1])
    mat_im = (mat_ref[1, 0], mat_ref[1, 1])
    wave_re, wave_im = halves(wave_re), halves(wave_im)
    half_re = dot3(wave_re, mat_re) - sign * dot3(wave_im, mat_im)
    half_im = dot3(wave_im, mat_re) + sign * dot3(wave_re, mat_im)
    half_re, half_im = halves(half_re), halves(half_im)
    return (
        dot3(mat_re, half_re) - sign * dot3(mat_im, half_im),
        dot3(mat_re, half_im) + sign * dot3(mat_im, half_re),
    )


def lanes(shape):
    return lax.broadcasted_iota(jnp.int32, shape, len(shape) - 1)


def turned(value, by):
    return pltpu.roll(value, by, value.ndim - 1)


def back_body(resid_ref, mat_ref, back_ref):
    back_ref[0], back_ref[1] = sandwich(mat_ref, 1.0, resid_ref[0], resid_ref[1])


def spread_body(off0, off1, off2, own_ref, near_ref, far_ref, up_ref, mid_ref, down_ref):
    tile = own_ref.shape[-1]
    for off, out_ref in ((off0, up_ref), (off1, mid_ref), (off2, down_ref)):
        left = off[0, 1]
        by = lax.select(left == 0, 0, tile - left)
        keep = lanes((tile, tile)) >= left
        for part in range(own_ref.shape[0]):
            out_ref[part, :, :tile] = turned(jnp.where(keep, own_ref[part], near_ref[part]), by)
            out_ref[part, :, tile:] = turned(jnp.where(keep, near_ref[part], far_ref[part]), by)


def rows_at(ref, start, count, width):
    rest = lax.rem(start, 8)
    value = ref[pl.ds(pl.multiple_of(start - rest, 8), count + 8), :width]
    value = value.reshape(count // 8 + 1, 8, value.shape[-1])
    value = pltpu.roll(value, lax.rem(8 - rest, 8), 1)
    keep = lax.broadcasted_iota(jnp.int32, value[1:].shape, 1) < 8 - rest
    return jnp.where(keep, value[:-1], value[1:]).reshape(count, value.shape[-1])


def rows_to(ref, start, value):
    count, width = value.shape
    rest = lax.rem(start, 8)
    value = pltpu.roll(value.reshape(count // 8, 8, width), rest, 1)
    none = jnp.zeros((1, 8, width), value.dtype)
    now, before = jnp.concatenate([value, none], axis=0), jnp.concatenate([none, value], axis=0)
    keep = lax.broadcasted_iota(jnp.int32, now.shape, 1) >= rest
    ref[pl.ds(pl.multiple_of(start - rest, 8), count + 8)] = jnp.where(keep, now, before).reshape(count + 8, width)


def windowed(tall_ref, top, up_ref, mid_ref, down_ref):
    tile, width = up_ref.shape[1:]
    for band, ref in enumerate((up_ref, mid_ref, down_ref)):
        tall_ref[:2, band * tile : (band + 1) * tile] = ref[...]
    return rows_at(tall_ref.at[0], top, width, width), rows_at(tall_ref.at[1], top, width, width)


def handed_out(tall_ref, top, terms, outs):
    tile, width = outs[0].shape[1:]
    zeros = jnp.zeros((tile, width), jnp.float32)
    for part, term in enumerate(terms):
        tall_ref[part, :tile] = zeros
        tall_ref[part, 2 * tile :] = zeros
        rows_to(tall_ref.at[part], top, term)
        for band, out_ref in enumerate(outs):
            out_ref[part] = tall_ref[part, band * tile : (band + 1) * tile]


def wave_body(
    off0, off1, off2, up_ref, mid_ref, down_ref, probe_ref, back_ref, mat_ref,
    out0, out1, out2, band0, band1, band2, tall_ref,
):
    top, left = off1[0, 0], off1[0, 1]
    trans_re, trans_im = windowed(tall_ref, top, up_ref, mid_ref, down_ref)
    probe_re, probe_im = probe_ref[0], probe_ref[1]
    wave_re, wave_im = sandwich(
        mat_ref, 1.0, probe_re * trans_re - probe_im * trans_im, probe_re * trans_im + probe_im * trans_re
    )
    back_re, back_im = back_ref[0], back_ref[1]
    terms = (wave_re * back_re + wave_im * back_im, wave_re * back_im - wave_im * back_re)
    handed_out(tall_ref, top, terms, (out0, out1, out2))
    width, tile = band0.shape
    light = wave_re * wave_re + wave_im * wave_im
    first, second = turned(light[:, :tile], left), turned(light[:, tile:], left)
    inside = lanes((width, tile)) >= left
    band0[...] = jnp.where(inside, first, 0.0)
    band1[:width] = jnp.where(inside, second, first)
    band2[:width] = jnp.where(inside, 0.0, second)
    row, lane = lax.broadcasted_iota(jnp.int32, (8, tile), 0), lanes((8, tile))
    extra = jnp.zeros((8, tile), jnp.float32)
    for along, off in enumerate((off0, off1, off2)):
        for axis in range(2):
            extra += jnp.where((row == along) & (lane == axis), off[0, axis].astype(jnp.float32), 0.0)
    band1[width:] = extra
    band2[width:] = extra


def pair_body(up_ref, own_ref, down_ref, out_ref):
    even = is_even()
    out_ref[0] = own_ref[...]
    out_ref[1] = jnp.where(even, up_ref[...], down_ref[...])


def pull_body(
    off1, up_ref, own_ref, down_ref, near_ref, near_swap_ref, far_ref, far_swap_ref,
    probe_ref, back_ref, mat_ref, out0, out1, out2, tall_ref,
):
    top, left = off1[0, 0], off1[0, 1]
    tile, width = own_ref.shape[-1], probe_ref.shape[-1]
    even = is_even()
    keep = lanes((width, tile)) < tile - left
    by = lax.select(left == 0, 0, tile - left)
    trans = []
    for part in range(2):
        tall_ref[part, :tile, :tile] = up_ref[part]
        tall_ref[part, tile : 2 * tile, :tile] = own_ref[part]
        tall_ref[part, 2 * tile :, :tile] = down_ref[part]
        first = turned(rows_at(tall_ref.at[part], top, width, tile), by)
        blocks = []
        for ref, swap_ref in ((near_ref, near_swap_ref), (far_ref, far_swap_ref)):
            tall_ref[part, :tile, :tile] = jnp.where(even, ref[1, part], swap_ref[part])
            tall_ref[part, tile : 2 * tile, :tile] = ref[0, part]
            tall_ref[part, 2 * tile :, :tile] = jnp.where(even, swap_ref[part], ref[1, part])
            blocks.append(turned(rows_at(tall_ref.at[part], top, width, tile), by))
        trans.append(
            jnp.concatenate([jnp.where(keep, first, blocks[0]), jnp.where(keep, blocks[0], blocks[1])], axis=1)
        )
    trans_re, trans_im = trans
    back_re, back_im = back_ref[0], back_ref[1]
    pulled_re, pulled_im = sandwich(
        mat_ref, -1.0, trans_re * back_re + trans_im * back_im, trans_re * back_im - trans_im * back_re
    )
    probe_re, probe_im = probe_ref[0], probe_ref[1]
    terms = (probe_re * pulled_re + probe_im * pulled_im, probe_re * pulled_im - probe_im * pulled_re)
    handed_out(tall_ref, top, terms, (out0, out1, out2))


def sent_offsets(ref):
    extra = ref[ref.shape[0] - 8 :]
    return [tuple(extra[along, axis].astype(jnp.int32) for axis in range(2)) for along in range(3)]


def fold_body(off1, band_ref, one_ref, two_ref, up_ref, mid_ref, down_ref, tall_ref):
    tile = up_ref.shape[0]
    width = band_ref.shape[0]
    zeros = jnp.zeros((tile, tile), jnp.float32)
    tops = (off1[0, 0], sent_offsets(one_ref)[1][0], sent_offsets(two_ref)[1][0])
    for slot, (top, ref) in enumerate(zip(tops, (band_ref, one_ref, two_ref))):
        tall_ref[slot, :tile] = zeros
        tall_ref[slot, 2 * tile :] = zeros
        rows_to(tall_ref.at[slot], top, ref[:width])
    for band, out_ref in enumerate((up_ref, mid_ref, down_ref)):
        rows = slice(band * tile, (band + 1) * tile)
        out_ref[...] = tall_ref[0, rows] + tall_ref[1, rows] + tall_ref[2, rows]


def merge_body(off0, off1, off2, above_ref, mid_ref, below_ref, out0, out1, out2):
    tile = out0.shape[-1]
    for part in range(out0.shape[0]):
        totals = [jnp.zeros((tile, tile), jnp.float32) for _ in range(3)]
        for off, ref in ((off0, above_ref), (off1, mid_ref), (off2, below_ref)):
            left = off[0, 1]
            first, second = turned(ref[part, :, :tile], left), turned(ref[part, :, tile:], left)
            inside = lanes((tile, tile)) >= left
            totals[0] += jnp.where(inside, first, 0.0)
            totals[1] += jnp.where(inside, second, first)
            totals[2] += jnp.where(inside, 0.0, second)
        out0[part], out1[part], out2[part] = totals


def bright_body(off0, off1, off2, one_ref, two_ref, probe_ref, out_ref, tall_ref):
    tile = out_ref.shape[-1]
    width = probe_ref.shape[-1]
    tall_ref[:tile] = jnp.zeros((tile, width), jnp.float32)
    tall_ref[tile + width :] = jnp.zeros((tile + 8, width), jnp.float32)
    tall_ref[tile : tile + width] = probe_ref[0] * probe_ref[0] + probe_ref[1] * probe_ref[1]
    own = [(off[0, 0], off[0, 1]) for off in (off0, off1, off2)]
    total = jnp.zeros((tile, tile), jnp.float32)
    for across, offs in enumerate((own, sent_offsets(one_ref), sent_offsets(two_ref))):
        for along, (top, left) in enumerate(offs):
            strip = rows_at(tall_ref, tile * (along + 1) - top, tile, width)
            inside = lanes((tile, tile)) >= left
            first, second = turned(strip[:, :tile], left), turned(strip[:, tile:], left)
            if across == 0:
                total += jnp.where(inside, first, 0.0)
            elif across == 1:
                total += jnp.where(inside, second, first)
            else:
                total += jnp.where(inside, 0.0, second)
    out_ref[...] = total


def final_body(
    own0_ref, own1_ref, here0_ref, there0_ref, here1_ref, there1_ref, light_ref, mid_ref, above_ref, below_ref, out_ref
):
    scale0 = STEP_SIZE / (light_ref[...] + REGULAR)
    scale1 = STEP_SIZE / (mid_ref[...] + above_ref[...] + below_ref[...] + REGULAR)
    for part in range(2):
        out_ref[0, part] = own0_ref[part] - (here0_ref[part] + there0_ref[part]) * scale0
        out_ref[1, part] = own1_ref[part] - (here1_ref[part] + there1_ref[part]) * scale1


def local(object_slices, probe, offsets, residuals):
    tile = object_slices.shape[-1]
    width = probe.shape[1]
    inverse, prop = tables(width)
    f32 = jnp.float32

    off = offsets.reshape(1, 2)
    off = [off, moved(off, "row", 1), moved(off, "row", 2)]
    resid = moved(residuals.reshape(2, width, width), "row", 1)
    (back,) = call(back_body, [((2, width, width), f32)], [resid, inverse])

    near = moved(object_slices[0], "col", -1)
    far = moved(near, "col", -1)
    strip = ((2, tile, width), f32)
    up, mid, down = call(spread_body, [strip] * 3, [*off, object_slices[0], near, far])
    first_strips = [moved(up, "row", 1), mid, moved(down, "row", -1)]

    own = object_slices[1]
    column = [moved(own, "row", 1), own, moved(own, "row", -1)]
    (pair,) = call(pair_body, [((2, 2, tile, tile), f32)], column)
    near = moved(pair, "col", -1)
    far = moved(near, "col", -1)
    second_strips = [*column, near, swapped(near[0]), far, swapped(far[0])]

    strips = [((2, tile, width), f32)] * 3
    bands = [((width, tile), f32), ((width + 8, tile), f32), ((width + 8, tile), f32)]
    tall = pltpu.VMEM((2, 3 * tile, width), f32)
    *waved, own, one, two = call(wave_body, strips + bands, [*off, *first_strips, probe, back, prop], [tall])
    one, two = moved(one, "col", 1), moved(two, "col", 2)
    pulled = call(pull_body, strips, [off[1], *second_strips, probe, back, prop], [tall])

    def shared(lifted):
        above, below = moved(lifted[0], "row", -1), moved(lifted[2], "row", 1)
        band = (2, tile, tile)
        first, second, third = call(merge_body, [(band, f32)] * 3, [*off, above, lifted[1], below])
        third = moved(third, "col", 1)
        third = second + third
        return first, moved(third, "col", 1)

    gradient1 = shared(waved)
    gradient0 = shared(pulled)

    up, mid, down = call(
        fold_body, [((tile, tile), f32)] * 3, [off[1], own, one, two], [pltpu.VMEM((3, 3 * tile, tile), f32)]
    )
    above, below = moved(up, "row", -1), moved(down, "row", 1)
    (light0,) = call(
        bright_body, [((tile, tile), f32)], [*off, one, two, probe],
        [pltpu.VMEM((2 * tile + width + 8, width), f32)],
    )

    (out,) = call(
        final_body, [(object_slices.shape, f32)],
        [object_slices[0], object_slices[1], *gradient0, *gradient1, light0, mid, above, below],
    )
    return out


def solution(mesh):
    split = (
        P(None, None, "row", "col"),
        P(),
        P("row", "col", None, None),
        P("row", "col", None, None, None, None),
    )

    return jax.shard_map(local, mesh=mesh, in_specs=split, out_specs=split[0], check_vma=False)
```
